32 devices in a mesh: rows: 8 (over z, x), cols: 4 (over y, core).
Axes of the slice: x: 2, y: 2, z: 4, core: 2. Of those that a mesh axis runs over, the one named last changes fastest.
Arguments:
- left_features: bfloat16 [2, 96, 512, 256], P(None, 'rows', 'cols'), may hold values from -6 to 6
- right_features: bfloat16 [2, 96, 512, 256], P(None, 'rows', 'cols'), may hold values from -6 to 6
- conv_weight: bfloat16 [3, 3, 256, 256], replicated, may hold values from -0.125 to 0.125
- conv_bias: float32 [256], replicated, may hold values from -3 to 3
Outputs:
- pyramid_out: float32 [2, 96, 512, 480], P(None, 'rows', 'cols')
The draws below stay inside these ranges and needn't reach their ends.
All inputs are finite; a program needn't handle non-finite values.
Results may differ from the reference program's by a relative error of at most 0.0012.
Values may be sent and summed in bfloat16 or wider, within the bound.
No kernel may reach another device: no remote copies, remote signals or barrier semaphores. Data moves between devices by JAX's collectives and lax.ppermute only.
A program may use at most 64 MiB of HBM per device.

```python
import math
import jax
import jax.numpy as jnp
from jax import lax

C = 256
DISP = 256
LEVELS = 4
B = 2
H_FEAT = 96
W_FEAT = 512


def steps_of(own_key, dims, pieces, low, largest):
    loudness, own = 1.0, jax.random.fold_in(own_key, 6)
    for position, shards_of in pieces:
        heights = jnp.exp(jax.random.uniform(jax.random.fold_in(own, position), (shards_of,), jnp.float32, low / len(pieces), largest / len(pieces)))
        loudness = loudness * jnp.repeat(heights, dims[position] // shards_of).reshape([-1 if axis == position else 1 for axis in range(len(dims))])
    return loudness


def noise(stream_key, extent, spread, reach, pieces=(), held_as=jnp.bfloat16):
    values = spread * jax.random.normal(stream_key, extent, jnp.float32)
    if pieces:
        values = values * steps_of(stream_key, extent, pieces, -0.22, 0.18)
    return jnp.clip(values, -reach, reach).astype(held_as)


def setup_inputs(seed: int = 0) -> dict:
    seeds = jax.random.split(jax.random.key(seed), 5)
    left_features = noise(seeds[0], (B, H_FEAT, W_FEAT, C), 1.0, 6.0, ((1, 8), (2, 4)))
    right_features = noise(seeds[1], (B, H_FEAT, W_FEAT, C), 1.0, 6.0, ((1, 8), (2, 4)))
    conv_weight = noise(seeds[2], (3, 3, C, C), (9 * C) ** -0.5, 0.125)
    conv_bias = noise(seeds[3], (C,), 0.5, 3.0, (), jnp.float32)
    return {"left_features": left_features, "right_features": right_features, "conv_weight": conv_weight, "conv_bias": conv_bias}


def conv_block(picture, conv_weight, conv_bias):
    height = picture.shape[0] - 2
    breadth = picture.shape[1] - 2
    channels = picture.shape[2]
    total = jnp.zeros((height * breadth, channels), jnp.float32)
    for row_tap in range(3):
        for col_tap in range(3):
            window = picture[row_tap:row_tap + height, col_tap:col_tap + breadth].reshape(-1, channels)
            total = total + jnp.dot(window, conv_weight[row_tap, col_tap], preferred_element_type=jnp.float32)
    centre = picture[1:-1, 1:-1].reshape(-1, channels).astype(jnp.float32)
    encoded = centre + jax.nn.relu(total + conv_bias.astype(jnp.float32))
    return encoded.astype(jnp.bfloat16).reshape(height, breadth, channels)

def pyramid(scores, span_count, level_count, channels):
    queries = scores.shape[-2]
    across = scores.shape[-1]
    leading = scores.shape[:-2]
    skewed = scores[..., 1:].reshape(leading + (-1,))
    skewed = jnp.pad(skewed, [(0, 0)] * len(leading) + [(0, queries)])
    skewed = skewed.reshape(leading + (queries, across))[..., :span_count][..., ::-1]
    volume = skewed * (1.0 / math.sqrt(channels))
    levels = [volume]
    for level in range(1, level_count):
        pooled = volume.reshape(leading + (queries, span_count >> level, 1 << level)).mean(axis=-1)
        levels.append(pooled)
    return jnp.concatenate(levels, axis=-1)

def reference(left_features, right_features, conv_weight, conv_bias):
    batch, height, breadth, channels = left_features.shape

    def encode(images):
        padded = jnp.pad(images, ((0, 0), (1, 1), (1, 1), (0, 0)))
        return lax.map(lambda picture: conv_block(picture, conv_weight, conv_bias), padded)
    left_out = encode(left_features)
    right_out = encode(right_features)
    right_padded = jnp.pad(right_out, ((0, 0), (0, 0), (DISP, 0), (0, 0)))
    left_rows = left_out.reshape(batch * height, breadth, channels)
    right_rows = right_padded.reshape(batch * height, DISP + breadth, channels)

    def one_row(pair):
        scores = jnp.dot(pair[0], pair[1].T, preferred_element_type=jnp.float32)
        return pyramid(scores, DISP, LEVELS, channels)
    result = lax.map(one_row, (left_rows, right_rows))
    return result.reshape(batch, height, breadth, -1)
```

```python
import math

import jax
import jax.numpy as jnp
from jax import lax
from jax.experimental import pallas as pl
from jax.experimental.pallas import tpu as pltpu
from jax.sharding import PartitionSpec as P

DISP = 256
LEVELS = 4
F32 = jnp.float32
BF16 = jnp.bfloat16
VMEM = pl.BlockSpec(memory_space=pltpu.VMEM)


def shifted(value, axis, steps):
    count = lax.axis_size(axis)
    first, last = max(0, -steps), min(count, count - steps)
    return lax.ppermute(value, axis, [(i, i + steps) for i in range(first, last)])


def iota(shape, dim):
    return lax.broadcasted_iota(jnp.int32, shape, dim)


def reversal(size):
    mirrored = iota((size, size), 0) + iota((size, size), 1) == size - 1
    return jnp.where(mirrored, 1.0, 0.0).astype(BF16)


def dot(a, b):
    return jnp.dot(a, b, preferred_element_type=F32)


def dot_t(a, b):
    return lax.dot_general(a, b, (((1,), (1,)), ((), ())), preferred_element_type=F32)


def cost(flops, nbytes):
    return pl.CostEstimate(flops=flops, bytes_accessed=nbytes, transcendentals=0)


def encode(image, side, edges, weight, bias, rows, which, mirror):
    batch, height, breadth, channels = image.shape
    count = len(rows)
    needed = sorted({r + dy for r in rows for dy in (-1, 0, 1)})
    place = {r: i for i, r in enumerate(needed)}

    def kernel(image_ref, before_ref, after_ref, *rest):
        if edges is None:
            weight_ref, bias_ref, out_ref, taps = rest
        else:
            up_ref, down_ref, weight_ref, bias_ref, out_ref, taps = rest
        spot = iota((breadth, channels), 0)
        for b in range(batch):
            for r in needed:
                if 0 <= r < height:
                    row = image_ref[b, r]
                    before = before_ref[which, b, r : r + 1, :]
                    after = after_ref[which, b, r : r + 1, :]
                else:
                    ref = up_ref if r < 0 else down_ref
                    row = ref[which, b, :breadth, :]
                    ends = ref[which, b, breadth:, :]
                    before = ends[0:1]
                    after = ends[1:2]
                wide = row.astype(F32)
                west = jnp.where(spot == 0, before.astype(F32), pltpu.roll(wide, 1, 0))
                east = jnp.where(
                    spot == breadth - 1, after.astype(F32), pltpu.roll(wide, breadth - 1, 0)
                )
                taps[place[r], :, :channels] = west.astype(BF16)
                taps[place[r], :, channels : 2 * channels] = row
                taps[place[r], :, 2 * channels :] = east.astype(BF16)
            total = None
            for dy in range(3):
                window = jnp.concatenate([taps[place[r + dy - 1]] for r in rows], axis=0)
                part = dot(window, weight_ref[dy])
                total = part if total is None else total + part
            centre = jnp.concatenate([image_ref[b, r] for r in rows], axis=0).astype(F32)
            encoded = (centre + jnp.maximum(total + bias_ref[...], 0.0)).astype(BF16)
            for i in range(count):
                value = encoded[i * breadth : (i + 1) * breadth]
                if mirror:
                    value = dot(reversal(breadth), value).astype(BF16)
                out_ref[b, i] = value

    operands = [image, side[0], side[1]] + ([] if edges is None else list(edges))
    operands += [weight.reshape(3, 3 * channels, channels), bias.reshape(1, channels)]
    return pl.pallas_call(
        kernel,
        out_shape=jax.ShapeDtypeStruct((batch, count, breadth, channels), BF16),
        in_specs=[VMEM] * len(operands),
        out_specs=VMEM,
        scratch_shapes=[pltpu.VMEM((len(needed), breadth, 3 * channels), BF16)],
        cost_estimate=cost(batch * count * breadth * channels * channels * 18, 2 * image.size),
        name="encode",
    )(*operands)


def triangle(left, right):
    batch, count, breadth, channels = left.shape

    def kernel(left_ref, right_ref, out_ref):
        near = iota((breadth, breadth), 1) > iota((breadth, breadth), 0)
        flip = reversal(breadth)
        for i in range(count):
            for b in range(0, batch, 2):
                upper = dot_t(left_ref[b, i], right_ref[b, i])
                upper = pltpu.roll(upper, 1, 1, stride=1, stride_axis=0)
                turned = dot(flip, left_ref[b + 1, i]).astype(BF16)
                lower = dot_t(turned, right_ref[b + 1, i])
                out_ref[b // 2, i] = jnp.where(near, upper, lower)

    return pl.pallas_call(
        kernel,
        out_shape=jax.ShapeDtypeStruct((batch // 2, count, breadth, breadth), F32),
        in_specs=[VMEM] * 2,
        out_specs=VMEM,
        cost_estimate=cost(2 * batch * count * breadth * breadth * channels, 4 * left.size),
        name="triangle",
    )(left, right)


def split(value):
    high = value.astype(BF16)
    return high, (value - high.astype(F32)).astype(BF16)


def volume(left, own, near, far, first, height, held):
    batch, count, breadth, channels = left.shape
    pooled = sum(DISP >> level for level in range(1, LEVELS))
    width = DISP + pooled
    scale = 1.0 / math.sqrt(channels)

    def kernel(*refs):
        left_ref, own_ref, near_ref, far_ref = refs[:4]
        out_ref = refs[-1]
        kept = iota((breadth, breadth), 1) > iota((breadth, breadth), 0)
        flip = reversal(breadth)
        source, target = iota((DISP, pooled), 0), iota((DISP, pooled), 1)
        pool = jnp.zeros((DISP, pooled), F32)
        start = 0
        for level in range(1, LEVELS):
            size = DISP >> level
            hit = (source >> level == target - start) & (target >= start) & (target < start + size)
            pool = jnp.where(hit, 1.0 / (1 << level), pool)
            start += size
        pool = pool.astype(BF16)
        for b in range(batch):
            window = jnp.concatenate([own_ref[b, 0], near_ref[b, 0]], axis=0)
            scores = dot_t(left_ref[b, 0], window)
            scores = pltpu.roll(scores, breadth + 1, 1, stride=1, stride_axis=0)
            corner = far_ref[b // 2, 0]
            if b % 2:
                high, low = split(corner)
                corner = dot(flip, high) + dot(flip, low)
                corner = pltpu.roll(corner, 1, 1, stride=1, stride_axis=0)
            tail = jnp.where(kept, corner, scores[:, breadth:])
            full = jnp.concatenate([scores[:, :breadth], tail], axis=1) * scale
            high, low = split(full)
            out_ref[b, 0, :, :DISP] = full
            out_ref[b, 0, :, DISP:] = dot(high, pool) + dot(low, pool)

    block = pl.BlockSpec((batch, 1, breadth, channels), lambda j: (0, j, 0, 0))
    operands = [left, own, near, far]
    specs = [block] * 3 + [pl.BlockSpec((batch // 2, 1, breadth, breadth), lambda j: (0, j, 0, 0))]
    aliases = {}
    if held is not None:
        operands.append(held)
        specs.append(pl.BlockSpec(memory_space=pl.ANY))
        aliases = {4: 0}
    return pl.pallas_call(
        kernel,
        grid=(count,),
        out_shape=jax.ShapeDtypeStruct((batch, height, breadth, width), F32),
        in_specs=specs,
        out_specs=pl.BlockSpec(
            (batch, 1, breadth, width), lambda j: (0, (j + first) % height, 0, 0)
        ),
        input_output_aliases=aliases,
        cost_estimate=cost(
            2 * batch * count * breadth * DISP * (channels + 2 * pooled),
            batch * count * breadth * (6 * channels + 4 * width),
        ),
        name="volume",
    )(*operands)


def shards(left_features, right_features, conv_weight, conv_bias):
    batch, height, breadth, channels = left_features.shape
    assert DISP == 2 * breadth and batch % 2 == 0
    both = (right_features, left_features)
    side = (
        shifted(jnp.stack([f[:, :, -1] for f in both]), "cols", 1),
        shifted(jnp.stack([f[:, :, 0] for f in both]), "cols", -1),
    )

    def edge(row):
        parts = [jnp.stack([f[:, row] for f in both])]
        parts += [s[:, :, row][:, :, None] for s in side]
        return jnp.concatenate(parts, axis=2)

    edges = (shifted(edge(-1), "rows", 1), shifted(edge(0), "rows", -1))
    half = height // 2
    groups = [list(range(1, 1 + half)), list(range(1 + half, height)) + [0]]
    weight, bias = conv_weight, conv_bias
    rights, lefts, nears, fars = [], [], [], []
    for rows in groups:
        outer = None if min(rows) > 0 and max(rows) < height - 1 else edges
        right = encode(right_features, side, outer, weight, bias, rows, 0, True)
        nears.append(shifted(right, "cols", 1))
        left = encode(left_features, side, outer, weight, bias, rows, 1, False)
        fars.append(shifted(left, "cols", -1))
        rights.append(right)
        lefts.append(left)
    corners = [shifted(triangle(l, r), "cols", 1) for l, r in zip(fars, nears)]
    out = None
    for k, rows in enumerate(groups):
        out = volume(lefts[k], rights[k], nears[k], corners[k], rows[0], height, out)
    return out


def solution(mesh):
    return jax.shard_map(
        shards,
        mesh=mesh,
        in_specs=(P(None, "rows", "cols", None), P(None, "rows", "cols", None), P(), P()),
        out_specs=P(None, "rows", "cols", None),
        check_vma=False,
    )
```

```python
import math

import jax
import jax.numpy as jnp
import numpy as np
from jax import lax
from jax.experimental import pallas as pl
from jax.experimental.pallas import tpu as pltpu
from jax.sharding import PartitionSpec as P

DISP = 256
LEVELS = 4
F32 = jnp.float32
BF16 = jnp.bfloat16


def shifted(value, axis, steps):
    count = lax.axis_size(axis)
    first, last = max(0, -steps), min(count, count - steps)
    return lax.ppermute(value, axis, [(i, i + steps) for i in range(first, last)])


def iota(shape, dim):
    return lax.broadcasted_iota(jnp.int32, shape, dim)


def reversal(size):
    mirrored = iota((size, size), 0) + iota((size, size), 1) == size - 1
    return jnp.where(mirrored, 1.0, 0.0).astype(BF16)


def dot(a, b):
    return jnp.dot(a, b, preferred_element_type=F32)


def dot_t(a, b):
    return lax.dot_general(a, b, (((1,), (1,)), ((), ())), preferred_element_type=F32)


def in_hbm(value):
    return pltpu.with_memory_space_constraint(value, pltpu.HBM)


def cost(flops, nbytes):
    return pl.CostEstimate(flops=flops, bytes_accessed=nbytes, transcendentals=0)


def encode(image, side, edges, weight, bias, rows, which, mirror):
    batch, height, breadth, channels = image.shape
    count = len(rows)
    needed = sorted({r + dy for r in rows for dy in (-1, 0, 1)})
    place = {r: i for i, r in enumerate(needed)}

    def kernel(image_ref, before_ref, after_ref, *rest):
        if edges is None:
            weight_ref, bias_ref, out_ref, taps = rest
        else:
            up_ref, down_ref, weight_ref, bias_ref, out_ref, taps = rest
        spot = iota((breadth, channels), 0)
        for r in needed:
            if 0 <= r < height:
                row = image_ref[0, r]
                before = before_ref[0, 0, r : r + 1, :]
                after = after_ref[0, 0, r : r + 1, :]
            else:
                ref = up_ref if r < 0 else down_ref
                row = ref[0, 0, :breadth, :]
                ends = ref[0, 0, breadth:, :]
                before = ends[0:1]
                after = ends[1:2]
            wide = row.astype(F32)
            west = jnp.where(spot == 0, before.astype(F32), pltpu.roll(wide, 1, 0))
            east = jnp.where(
                spot == breadth - 1, after.astype(F32), pltpu.roll(wide, breadth - 1, 0)
            )
            taps[place[r], :, :channels] = west.astype(BF16)
            taps[place[r], :, channels : 2 * channels] = row
            taps[place[r], :, 2 * channels :] = east.astype(BF16)
        total = None
        for dy in range(3):
            window = jnp.concatenate([taps[place[r + dy - 1]] for r in rows], axis=0)
            part = dot(window, weight_ref[dy])
            total = part if total is None else total + part
        centre = jnp.concatenate([image_ref[0, r] for r in rows], axis=0).astype(F32)
        encoded = (centre + jnp.maximum(total + bias_ref[...], 0.0)).astype(BF16)
        values = [encoded[i * breadth : (i + 1) * breadth] for i in range(count)]
        if mirror:
            flip = reversal(breadth)
            values = [dot(flip, value).astype(BF16) for value in values]
        for i in range(count):
            out_ref[0, i] = values[i]

    operands = [image, side[0], side[1]] + ([] if edges is None else list(edges))
    operands += [weight.reshape(3, 3 * channels, channels), bias.reshape(1, channels)]
    picked = [pl.BlockSpec((1, 1) + a.shape[2:], lambda b: (which, b, 0, 0)) for a in operands[1:-2]]
    return pl.pallas_call(
        kernel,
        grid=(batch,),
        out_shape=jax.ShapeDtypeStruct((batch, count, breadth, channels), BF16),
        in_specs=[pl.BlockSpec((1, height, breadth, channels), lambda b: (b, 0, 0, 0))]
        + picked
        + [
            pl.BlockSpec((3, 3 * channels, channels), lambda b: (0, 0, 0)),
            pl.BlockSpec((1, channels), lambda b: (0, 0)),
        ],
        out_specs=pl.BlockSpec((1, count, breadth, channels), lambda b: (b, 0, 0, 0)),
        scratch_shapes=[pltpu.VMEM((len(needed), breadth, 3 * channels), BF16)],
        cost_estimate=cost(batch * count * breadth * channels * channels * 18, 2 * image.size),
        name="encode",
    )(*operands)


def triangle(left, right):
    batch, count, breadth, channels = left.shape

    def kernel(left_ref, right_ref, out_ref):
        near = iota((breadth, breadth), 1) > iota((breadth, breadth), 0)
        flip = reversal(breadth)
        for i in range(2):
            for b in range(0, batch, 2):
                upper = dot_t(left_ref[b, i], right_ref[b, i])
                upper = pltpu.roll(upper, 1, 1, stride=1, stride_axis=0)
                turned = dot(flip, left_ref[b + 1, i]).astype(BF16)
                lower = dot_t(turned, right_ref[b + 1, i])
                out_ref[b // 2, i] = jnp.where(near, upper, lower)

    return pl.pallas_call(
        kernel,
        grid=(count // 2,),
        out_shape=jax.ShapeDtypeStruct((batch // 2, count, breadth, breadth), F32),
        in_specs=[pl.BlockSpec((batch, 2, breadth, channels), lambda j: (0, j, 0, 0))] * 2,
        out_specs=pl.BlockSpec((batch // 2, 2, breadth, breadth), lambda j: (0, j, 0, 0)),
        cost_estimate=cost(2 * batch * count * breadth * breadth * channels, 4 * left.size),
        name="triangle",
    )(in_hbm(left), in_hbm(right))


def split(value):
    high = value.astype(BF16)
    return high, (value - high.astype(F32)).astype(BF16)


def pooling():
    rows = [np.zeros((0, DISP), np.float32)]
    for level in range(1, LEVELS):
        size = DISP >> level
        groups = np.arange(DISP)[None, :] >> level == np.arange(size)[:, None]
        rows.append(groups.astype(np.float32) / (1 << level))
    return np.concatenate(rows, axis=0)


def volume(left, own, near, far, first, height, held):
    batch, count, breadth, channels = left.shape
    pool = jnp.asarray(pooling(), BF16)
    pooled = pool.shape[0]
    width = DISP + pooled
    scale = 1.0 / math.sqrt(channels)

    def kernel(*refs):
        left_ref, own_ref, near_ref, far_ref, pool_ref = refs[:5]
        out_ref = refs[-1]
        kept = iota((breadth, breadth), 1) > iota((breadth, breadth), 0)
        flip = reversal(breadth)
        spots = [(b, i) for i in range(2) for b in range(batch)]
        scores, corners, fulls = {}, {}, {}
        for b, i in spots:
            window = jnp.concatenate([own_ref[b, i], near_ref[b, i]], axis=0)
            scores[b, i] = dot_t(left_ref[b, i], window)
        for b, i in spots:
            corners[b, i] = far_ref[b // 2, i]
            if b % 2:
                high, low = split(corners[b, i])
                corners[b, i] = dot(flip, high) + dot(flip, low)
        for b, i in spots:
            turned = pltpu.roll(scores[b, i], breadth + 1, 1, stride=1, stride_axis=0)
            corner = corners[b, i]
            if b % 2:
                corner = pltpu.roll(corner, 1, 1, stride=1, stride_axis=0)
            tail = jnp.where(kept, corner, turned[:, breadth:])
            fulls[b, i] = jnp.concatenate([turned[:, :breadth], tail], axis=1) * scale
        for i in range(2):
            for b in range(0, batch, 2):
                high, low = split(jnp.concatenate([fulls[b, i], fulls[b + 1, i]], axis=0))
                means = dot_t(pool_ref[...], high) + dot_t(pool_ref[...], low)
                out_ref[b, i, DISP:, :] = means[:, :breadth]
                out_ref[b + 1, i, DISP:, :] = means[:, breadth:]
        for b, i in spots:
            out_ref[b, i, :DISP, :] = fulls[b, i].T

    block = pl.BlockSpec((batch, 2, breadth, channels), lambda j: (0, j, 0, 0))
    operands = [left, own, in_hbm(near), in_hbm(far), pool]
    specs = [block] * 3 + [pl.BlockSpec((batch // 2, 2, breadth, breadth), lambda j: (0, j, 0, 0))]
    specs.append(pl.BlockSpec((pooled, DISP), lambda j: (0, 0)))
    aliases = {}
    if held is not None:
        operands.append(held)
        specs.append(pl.BlockSpec(memory_space=pl.ANY))
        aliases = {5: 0}
    return pl.pallas_call(
        kernel,
        grid=(count // 2,),
        out_shape=jax.ShapeDtypeStruct((batch, height, width, breadth), F32),
        in_specs=specs,
        out_specs=pl.BlockSpec(
            (batch, 2, width, breadth), lambda j: (0, (j + first // 2) % (height // 2), 0, 0)
        ),
        input_output_aliases=aliases,
        cost_estimate=cost(
            2 * batch * count * breadth * DISP * (channels + 2 * pooled),
            batch * count * breadth * (6 * channels + 4 * width),
        ),
        name="volume",
    )(*operands)


def shards(left_features, right_features, conv_weight, conv_bias):
    batch, height, breadth, channels = left_features.shape
    assert DISP == 2 * breadth and batch % 2 == 0 and height % 4 == 0
    both = (right_features, left_features)
    side = (
        shifted(jnp.stack([f[:, :, -1] for f in both]), "cols", 1),
        shifted(jnp.stack([f[:, :, 0] for f in both]), "cols", -1),
    )

    def edge(row):
        parts = [jnp.stack([f[:, row] for f in both])]
        parts += [s[:, :, row][:, :, None] for s in side]
        return jnp.concatenate(parts, axis=2)

    edges = (shifted(edge(-1), "rows", 1), shifted(edge(0), "rows", -1))
    half = height // 2
    groups = [list(range(2, 2 + half)), list(range(2 + half, height)) + [0, 1]]
    weight, bias = conv_weight, conv_bias
    rights, lefts, nears, fars = [], [], [], []
    for rows in groups:
        outer = None if min(rows) > 0 and max(rows) < height - 1 else edges
        right = encode(right_features, side, outer, weight, bias, rows, 0, True)
        nears.append(shifted(right, "cols", 1))
        left = encode(left_features, side, outer, weight, bias, rows, 1, False)
        fars.append(shifted(left, "cols", -1))
        rights.append(right)
        lefts.append(left)
    corners = [shifted(triangle(l, r), "cols", 1) for l, r in zip(fars, nears)]
    out = None
    for k, rows in enumerate(groups):
        out = volume(lefts[k], rights[k], nears[k], corners[k], rows[0], height, out)
    return jnp.swapaxes(out, 2, 3)


def solution(mesh):
    return jax.shard_map(
        shards,
        mesh=mesh,
        in_specs=(P(None, "rows", "cols", None), P(None, "rows", "cols", None), P(), P()),
        out_specs=P(None, "rows", "cols", None),
        check_vma=False,
    )
```

```python
import math

import jax
import jax.numpy as jnp
import numpy as np
from jax import lax
from jax.experimental import pallas as pl
from jax.experimental.pallas import tpu as pltpu
from jax.sharding import PartitionSpec as P

DISP = 256
LEVELS = 4
F32 = jnp.float32
BF16 = jnp.bfloat16


def shifted(value, axis, steps):
    count = lax.axis_size(axis)
    first, last = max(0, -steps), min(count, count - steps)
    return lax.ppermute(value, axis, [(i, i + steps) for i in range(first, last)])


def iota(shape, dim):
    return lax.broadcasted_iota(jnp.int32, shape, dim)


def reversal(size):
    mirrored = iota((size, size), 0) + iota((size, size), 1) == size - 1
    return jnp.where(mirrored, 1.0, 0.0).astype(BF16)


def dot(a, b):
    return jnp.dot(a, b, preferred_element_type=F32)


def dot_t(a, b):
    return lax.dot_general(a, b, (((1,), (1,)), ((), ())), preferred_element_type=F32)


FULL = pltpu.CompilerParams(vmem_limit_bytes=67043328)


def in_hbm(value):
    return pltpu.with_memory_space_constraint(value, pltpu.HBM)


def cost(flops, nbytes):
    return pl.CostEstimate(flops=flops, bytes_accessed=nbytes, transcendentals=0)


def encode(image, side, edges, weight, bias, rows, which, mirror):
    batch, height, breadth, channels = image.shape
    count = len(rows)
    needed = sorted({r + dy for r in rows for dy in (-1, 0, 1)})
    place = {r: i for i, r in enumerate(needed)}

    def kernel(image_ref, before_ref, after_ref, *rest):
        if edges is None:
            weight_ref, bias_ref, out_ref, taps = rest
        else:
            up_ref, down_ref, weight_ref, bias_ref, out_ref, taps = rest
        spot = iota((breadth, channels), 0)
        for r in needed:
            if 0 <= r < height:
                row = image_ref[0, r]
                before = before_ref[0, 0, r : r + 1, :]
                after = after_ref[0, 0, r : r + 1, :]
            else:
                ref = up_ref if r < 0 else down_ref
                row = ref[0, 0, :breadth, :]
                ends = ref[0, 0, breadth:, :]
                before = ends[0:1]
                after = ends[1:2]
            wide = row.astype(F32)
            west = jnp.where(spot == 0, before.astype(F32), pltpu.roll(wide, 1, 0))
            east = jnp.where(
                spot == breadth - 1, after.astype(F32), pltpu.roll(wide, breadth - 1, 0)
            )
            taps[place[r], :, :channels] = west.astype(BF16)
            taps[place[r], :, channels : 2 * channels] = row
            taps[place[r], :, 2 * channels :] = east.astype(BF16)
        total = None
        for dy in range(3):
            window = jnp.concatenate([taps[place[r + dy - 1]] for r in rows], axis=0)
            part = dot(window, weight_ref[dy])
            total = part if total is None else total + part
        centre = jnp.concatenate([image_ref[0, r] for r in rows], axis=0).astype(F32)
        encoded = (centre + jnp.maximum(total + bias_ref[...], 0.0)).astype(BF16)
        values = [encoded[i * breadth : (i + 1) * breadth] for i in range(count)]
        if mirror:
            flip = reversal(breadth)
            values = [dot(flip, value).astype(BF16) for value in values]
        for i in range(count):
            out_ref[0, i] = values[i]

    operands = [image, side[0], side[1]] + ([] if edges is None else list(edges))
    operands += [weight.reshape(3, 3 * channels, channels), bias.reshape(1, channels)]
    picked = [pl.BlockSpec((1, 1) + a.shape[2:], lambda b: (which, b, 0, 0)) for a in operands[1:-2]]
    return pl.pallas_call(
        kernel,
        grid=(batch,),
        out_shape=jax.ShapeDtypeStruct((batch, count, breadth, channels), BF16),
        in_specs=[pl.BlockSpec((1, height, breadth, channels), lambda b: (b, 0, 0, 0))]
        + picked
        + [
            pl.BlockSpec((3, 3 * channels, channels), lambda b: (0, 0, 0)),
            pl.BlockSpec((1, channels), lambda b: (0, 0)),
        ],
        out_specs=pl.BlockSpec((1, count, breadth, channels), lambda b: (b, 0, 0, 0)),
        scratch_shapes=[pltpu.VMEM((len(needed), breadth, 3 * channels), BF16)],
        cost_estimate=cost(batch * count * breadth * channels * channels * 18, 2 * image.size),
        compiler_params=FULL,
        name="encode",
    )(*operands)


def triangle(left, right):
    batch, count, breadth, channels = left.shape

    def kernel(left_ref, right_ref, out_ref):
        near = iota((breadth, breadth), 1) > iota((breadth, breadth), 0)
        flip = reversal(breadth)
        spots = [(b, i) for i in range(2) for b in range(0, batch, 2)]
        turned = [dot(flip, left_ref[b + 1, i]).astype(BF16) for b, i in spots]
        upper = [dot_t(left_ref[b, i], right_ref[b, i]) for b, i in spots]
        lower = [dot_t(t, right_ref[b + 1, i]) for t, (b, i) in zip(turned, spots)]
        upper = [pltpu.roll(u, 1, 1, stride=1, stride_axis=0) for u in upper]
        for k, (b, i) in enumerate(spots):
            out_ref[b // 2, i] = jnp.where(near, upper[k], lower[k])

    return pl.pallas_call(
        kernel,
        grid=(count // 2,),
        out_shape=jax.ShapeDtypeStruct((batch // 2, count, breadth, breadth), F32),
        in_specs=[pl.BlockSpec((batch, 2, breadth, channels), lambda j: (0, j, 0, 0))] * 2,
        out_specs=pl.BlockSpec((batch // 2, 2, breadth, breadth), lambda j: (0, j, 0, 0)),
        cost_estimate=cost(2 * batch * count * breadth * breadth * channels, 4 * left.size),
        compiler_params=FULL,
        name="triangle",
    )(in_hbm(left), in_hbm(right))


def split(value):
    high = value.astype(BF16)
    return high, (value - high.astype(F32)).astype(BF16)


def pooling():
    rows = [np.zeros((0, DISP), np.float32)]
    for level in range(1, LEVELS):
        size = DISP >> level
        groups = np.arange(DISP)[None, :] >> level == np.arange(size)[:, None]
        rows.append(groups.astype(np.float32) / (1 << level))
    return np.concatenate(rows, axis=0)


def volume(left, own, near, far, first, height, held):
    batch, count, breadth, channels = left.shape
    pool = jnp.asarray(pooling(), BF16)
    pooled = pool.shape[0]
    width = DISP + pooled
    scale = 1.0 / math.sqrt(channels)

    def kernel(*refs):
        left_ref, own_ref, near_ref, far_ref, pool_ref = refs[:5]
        out_ref = refs[-1]
        kept = iota((breadth, breadth), 1) > iota((breadth, breadth), 0)
        flip = reversal(breadth)
        spots = [(b, i) for i in range(2) for b in range(batch)]
        scores, corners, fulls = {}, {}, {}
        for b, i in spots:
            window = jnp.concatenate([own_ref[b, i], near_ref[b, i]], axis=0)
            scores[b, i] = dot_t(left_ref[b, i], window)
        for b, i in spots:
            corners[b, i] = far_ref[b // 2, i]
            if b % 2:
                high, low = split(corners[b, i])
                corners[b, i] = dot(flip, high) + dot(flip, low)
        for b, i in spots:
            turned = pltpu.roll(scores[b, i], breadth + 1, 1, stride=1, stride_axis=0)
            corner = corners[b, i]
            if b % 2:
                corner = pltpu.roll(corner, 1, 1, stride=1, stride_axis=0)
            tail = jnp.where(kept, corner, turned[:, breadth:])
            fulls[b, i] = jnp.concatenate([turned[:, :breadth], tail], axis=1) * scale
        for i in range(2):
            for b in range(0, batch, 2):
                high, low = split(jnp.concatenate([fulls[b, i], fulls[b + 1, i]], axis=0))
                means = dot_t(pool_ref[...], high) + dot_t(pool_ref[...], low)
                out_ref[b, i, DISP:, :] = means[:, :breadth]
                out_ref[b + 1, i, DISP:, :] = means[:, breadth:]
        for b, i in spots:
            out_ref[b, i, :DISP, :] = fulls[b, i].T

    block = pl.BlockSpec((batch, 2, breadth, channels), lambda j: (0, j, 0, 0))
    operands = [left, own, in_hbm(near), in_hbm(far), pool]
    specs = [block] * 3 + [pl.BlockSpec((batch // 2, 2, breadth, breadth), lambda j: (0, j, 0, 0))]
    specs.append(pl.BlockSpec((pooled, DISP), lambda j: (0, 0)))
    aliases = {}
    if held is not None:
        operands.append(held)
        specs.append(pl.BlockSpec(memory_space=pl.ANY))
        aliases = {5: 0}
    return pl.pallas_call(
        kernel,
        grid=(count // 2,),
        out_shape=jax.ShapeDtypeStruct((batch, height, width, breadth), F32),
        in_specs=specs,
        out_specs=pl.BlockSpec(
            (batch, 2, width, breadth), lambda j: (0, (j + first // 2) % (height // 2), 0, 0)
        ),
        input_output_aliases=aliases,
        cost_estimate=cost(
            2 * batch * count * breadth * DISP * (channels + 2 * pooled),
            batch * count * breadth * (6 * channels + 4 * width),
        ),
        compiler_params=FULL,
        name="volume",
    )(*operands)


def shards(left_features, right_features, conv_weight, conv_bias):
    batch, height, breadth, channels = left_features.shape
    assert DISP == 2 * breadth and batch % 2 == 0 and height % 4 == 0
    both = (right_features, left_features)
    side = (
        shifted(jnp.stack([f[:, :, -1] for f in both]), "cols", 1),
        shifted(jnp.stack([f[:, :, 0] for f in both]), "cols", -1),
    )

    def edge(row):
        parts = [jnp.stack([f[:, row] for f in both])]
        parts += [s[:, :, row][:, :, None] for s in side]
        return jnp.concatenate(parts, axis=2)

    edges = (shifted(edge(-1), "rows", 1), shifted(edge(0), "rows", -1))
    half = height // 2
    groups = [list(range(2, 2 + half)), list(range(2 + half, height)) + [0, 1]]
    weight, bias = conv_weight, conv_bias
    rights, lefts, nears, fars = [], [], [], []
    for rows in groups:
        outer = None if min(rows) > 0 and max(rows) < height - 1 else edges
        right = encode(right_features, side, outer, weight, bias, rows, 0, True)
        nears.append(shifted(right, "cols", 1))
        left = encode(left_features, side, outer, weight, bias, rows, 1, False)
        fars.append(shifted(left, "cols", -1))
        rights.append(right)
        lefts.append(left)
    corners = [shifted(triangle(l, r), "cols", 1) for l, r in zip(fars, nears)]
    out = None
    for k, rows in enumerate(groups):
        out = volume(lefts[k], rights[k], nears[k], corners[k], rows[0], height, out)
    return jnp.swapaxes(out, 2, 3)


def solution(mesh):
    return jax.shard_map(
        shards,
        mesh=mesh,
        in_specs=(P(None, "rows", "cols", None), P(None, "rows", "cols", None), P(), P()),
        out_specs=P(None, "rows", "cols", None),
        check_vma=False,
    )
```

```python
import math

import jax
import jax.numpy as jnp
import numpy as np
from jax import lax
from jax.experimental import pallas as pl
from jax.experimental.pallas import tpu as pltpu
from jax.sharding import PartitionSpec as P

DISP = 256
LEVELS = 4
F32 = jnp.float32
BF16 = jnp.bfloat16


def shifted(value, axis, steps):
    count = lax.axis_size(axis)
    first, last = max(0, -steps), min(count, count - steps)
    return lax.ppermute(value, axis, [(i, i + steps) for i in range(first, last)])


def iota(shape, dim):
    return lax.broadcasted_iota(jnp.int32, shape, dim)


def reversal(size):
    mirrored = iota((size, size), 0) + iota((size, size), 1) == size - 1
    return jnp.where(mirrored, 1.0, 0.0).astype(BF16)


def dot(a, b):
    return jnp.dot(a, b, preferred_element_type=F32)


def dot_t(a, b):
    return lax.dot_general(a, b, (((1,), (1,)), ((), ())), preferred_element_type=F32)


FULL = pltpu.CompilerParams(vmem_limit_bytes=67043328)


def in_hbm(value):
    return pltpu.with_memory_space_constraint(value, pltpu.HBM)


def cost(flops, nbytes):
    return pl.CostEstimate(flops=flops, bytes_accessed=nbytes, transcendentals=0)


def encode(image, side, edges, weight, bias, rows, which, mirror):
    batch, height, breadth, channels = image.shape
    count = len(rows)
    needed = sorted({r + dy for r in rows for dy in (-1, 0, 1)})
    place = {r: i for i, r in enumerate(needed)}

    def kernel(image_ref, before_ref, after_ref, *rest):
        if edges is None:
            weight_ref, bias_ref, out_ref, taps = rest
        else:
            up_ref, down_ref, weight_ref, bias_ref, out_ref, taps = rest
        spot = iota((breadth, channels), 0)
        for r in needed:
            if 0 <= r < height:
                row = image_ref[0, r]
                before = before_ref[0, 0, r : r + 1, :]
                after = after_ref[0, 0, r : r + 1, :]
            else:
                ref = up_ref if r < 0 else down_ref
                row = ref[0, 0, :breadth, :]
                ends = ref[0, 0, breadth:, :]
                before = ends[0:1]
                after = ends[1:2]
            wide = row.astype(F32)
            west = jnp.where(spot == 0, before.astype(F32), pltpu.roll(wide, 1, 0))
            east = jnp.where(
                spot == breadth - 1, after.astype(F32), pltpu.roll(wide, breadth - 1, 0)
            )
            taps[place[r], :, :channels] = west.astype(BF16)
            taps[place[r], :, channels : 2 * channels] = row
            taps[place[r], :, 2 * channels :] = east.astype(BF16)
        total = None
        for dy in range(3):
            window = jnp.concatenate([taps[place[r + dy - 1]] for r in rows], axis=0)
            part = dot(window, weight_ref[dy])
            total = part if total is None else total + part
        centre = jnp.concatenate([image_ref[0, r] for r in rows], axis=0).astype(F32)
        encoded = (centre + jnp.maximum(total + bias_ref[...], 0.0)).astype(BF16)
        values = [encoded[i * breadth : (i + 1) * breadth] for i in range(count)]
        if mirror:
            flip = reversal(breadth)
            values = [dot(flip, value).astype(BF16) for value in values]
        for i in range(count):
            out_ref[0, i] = values[i]

    operands = [image, side[0], side[1]] + ([] if edges is None else list(edges))
    operands += [weight.reshape(3, 3 * channels, channels), bias.reshape(1, channels)]
    picked = [pl.BlockSpec((1, 1) + a.shape[2:], lambda b: (which, b, 0, 0)) for a in operands[1:-2]]
    return pl.pallas_call(
        kernel,
        grid=(batch,),
        out_shape=jax.ShapeDtypeStruct((batch, count, breadth, channels), BF16),
        in_specs=[pl.BlockSpec((1, height, breadth, channels), lambda b: (b, 0, 0, 0))]
        + picked
        + [
            pl.BlockSpec((3, 3 * channels, channels), lambda b: (0, 0, 0)),
            pl.BlockSpec((1, channels), lambda b: (0, 0)),
        ],
        out_specs=pl.BlockSpec((1, count, breadth, channels), lambda b: (b, 0, 0, 0)),
        scratch_shapes=[pltpu.VMEM((len(needed), breadth, 3 * channels), BF16)],
        cost_estimate=cost(batch * count * breadth * channels * channels * 18, 2 * image.size),
        compiler_params=None if edges is None else FULL,
        name="encode",
    )(*operands)


def triangle(left, right):
    batch, count, breadth, channels = left.shape

    def kernel(left_ref, right_ref, out_ref):
        near = iota((breadth, breadth), 1) > iota((breadth, breadth), 0)
        flip = reversal(breadth)
        spots = [(b, i) for i in range(2) for b in range(0, batch, 2)]
        turned = [dot(flip, left_ref[b + 1, i]).astype(BF16) for b, i in spots]
        upper = [dot_t(left_ref[b, i], right_ref[b, i]) for b, i in spots]
        lower = [dot_t(t, right_ref[b + 1, i]) for t, (b, i) in zip(turned, spots)]
        upper = [pltpu.roll(u, 1, 1, stride=1, stride_axis=0) for u in upper]
        for k, (b, i) in enumerate(spots):
            out_ref[b // 2, i] = jnp.where(near, upper[k], lower[k])

    return pl.pallas_call(
        kernel,
        grid=(count // 2,),
        out_shape=jax.ShapeDtypeStruct((batch // 2, count, breadth, breadth), F32),
        in_specs=[pl.BlockSpec((batch, 2, breadth, channels), lambda j: (0, j, 0, 0))] * 2,
        out_specs=pl.BlockSpec((batch // 2, 2, breadth, breadth), lambda j: (0, j, 0, 0)),
        cost_estimate=cost(2 * batch * count * breadth * breadth * channels, 4 * left.size),
        compiler_params=FULL,
        name="triangle",
    )(in_hbm(left), in_hbm(right))


def split(value):
    high = value.astype(BF16)
    return high, (value - high.astype(F32)).astype(BF16)


def pooling():
    rows = [np.zeros((0, DISP), np.float32)]
    for level in range(1, LEVELS):
        size = DISP >> level
        groups = np.arange(DISP)[None, :] >> level == np.arange(size)[:, None]
        rows.append(groups.astype(np.float32) / (1 << level))
    return np.concatenate(rows, axis=0)


def volume(left, own, near, far, first, height, held):
    batch, count, breadth, channels = left.shape
    pool = jnp.asarray(pooling(), BF16)
    pooled = pool.shape[0]
    width = DISP + pooled
    scale = 1.0 / math.sqrt(channels)

    def kernel(*refs):
        left_ref, own_ref, near_ref, far_ref, pool_ref = refs[:5]
        out_ref = refs[-1]
        kept = iota((breadth, breadth), 1) > iota((breadth, breadth), 0)
        flip = reversal(breadth)
        spots = [(b, i) for i in range(2) for b in range(batch)]
        scores, corners, fulls = {}, {}, {}
        for b, i in spots:
            window = jnp.concatenate([own_ref[b, i], near_ref[b, i]], axis=0)
            scores[b, i] = dot_t(left_ref[b, i], window)
        for b, i in spots:
            corners[b, i] = far_ref[b // 2, i]
            if b % 2:
                high, low = split(corners[b, i])
                corners[b, i] = dot(flip, high) + dot(flip, low)
        for b, i in spots:
            turned = pltpu.roll(scores[b, i], breadth + 1, 1, stride=1, stride_axis=0)
            corner = corners[b, i]
            if b % 2:
                corner = pltpu.roll(corner, 1, 1, stride=1, stride_axis=0)
            tail = jnp.where(kept, corner, turned[:, breadth:])
            fulls[b, i] = jnp.concatenate([turned[:, :breadth], tail], axis=1) * scale
        for i in range(2):
            for b in range(0, batch, 2):
                high, low = split(jnp.concatenate([fulls[b, i], fulls[b + 1, i]], axis=0))
                means = dot_t(pool_ref[...], high) + dot_t(pool_ref[...], low)
                out_ref[b, i, DISP:, :] = means[:, :breadth]
                out_ref[b + 1, i, DISP:, :] = means[:, breadth:]
        for b, i in spots:
            out_ref[b, i, :DISP, :] = fulls[b, i].T

    block = pl.BlockSpec((batch, 2, breadth, channels), lambda j: (0, j, 0, 0))
    operands = [left, own, in_hbm(near), in_hbm(far), pool]
    specs = [block] * 3 + [pl.BlockSpec((batch // 2, 2, breadth, breadth), lambda j: (0, j, 0, 0))]
    specs.append(pl.BlockSpec((pooled, DISP), lambda j: (0, 0)))
    aliases = {}
    if held is not None:
        operands.append(held)
        specs.append(pl.BlockSpec(memory_space=pl.ANY))
        aliases = {5: 0}
    return pl.pallas_call(
        kernel,
        grid=(count // 2,),
        out_shape=jax.ShapeDtypeStruct((batch, height, width, breadth), F32),
        in_specs=specs,
        out_specs=pl.BlockSpec(
            (batch, 2, width, breadth), lambda j: (0, (j + first // 2) % (height // 2), 0, 0)
        ),
        input_output_aliases=aliases,
        cost_estimate=cost(
            2 * batch * count * breadth * DISP * (channels + 2 * pooled),
            batch * count * breadth * (6 * channels + 4 * width),
        ),
        compiler_params=FULL,
        name="volume",
    )(*operands)


def shards(left_features, right_features, conv_weight, conv_bias):
    batch, height, breadth, channels = left_features.shape
    assert DISP == 2 * breadth and batch % 2 == 0 and height % 4 == 0
    both = (right_features, left_features)
    side = (
        shifted(jnp.stack([f[:, :, -1] for f in both]), "cols", 1),
        shifted(jnp.stack([f[:, :, 0] for f in both]), "cols", -1),
    )

    def edge(row):
        parts = [jnp.stack([f[:, row] for f in both])]
        parts += [s[:, :, row][:, :, None] for s in side]
        return jnp.concatenate(parts, axis=2)

    edges = (shifted(edge(-1), "rows", 1), shifted(edge(0), "rows", -1))
    half = height // 2
    groups = [list(range(2, 2 + half)), list(range(2 + half, height)) + [0, 1]]
    weight, bias = conv_weight, conv_bias
    rights, lefts, nears, fars = [], [], [], []
    for rows in groups:
        outer = None if min(rows) > 0 and max(rows) < height - 1 else edges
        right = encode(right_features, side, outer, weight, bias, rows, 0, True)
        nears.append(shifted(right, "cols", 1))
        left = encode(left_features, side, outer, weight, bias, rows, 1, False)
        fars.append(shifted(left, "cols", -1))
        rights.append(right)
        lefts.append(left)
    corners = [shifted(triangle(l, r), "cols", 1) for l, r in zip(fars, nears)]
    out = None
    for k, rows in enumerate(groups):
        out = volume(lefts[k], rights[k], nears[k], corners[k], rows[0], height, out)
    return jnp.swapaxes(out, 2, 3)


def solution(mesh):
    return jax.shard_map(
        shards,
        mesh=mesh,
        in_specs=(P(None, "rows", "cols", None), P(None, "rows", "cols", None), P(), P()),
        out_specs=P(None, "rows", "cols", None),
        check_vma=False,
    )
```
